32 devices in a mesh: row: 16 (over z, y, core), col: 2 (over x).
Axes of the slice: x: 2, y: 2, z: 4, core: 2. Of those that a mesh axis runs over, the one named last changes fastest.
Arguments:
- images: bfloat16 [2048, 1024], P(('row', 'col')), as said below
- texts: bfloat16 [2048, 1024], P(('row', 'col')), as said below
- matches: int32 [2048], P('row'), may hold values from 0 to 2047, each once
- logit_scale: float32 [], replicated, may hold values from 20 to 400
Outputs:
- loss: float32 [], replicated
- image_grad: float32 [2048, 1024], P(('row', 'col'))
- text_grad: float32 [2048, 1024], P(('row', 'col'))
The draws below stay inside these ranges and needn't reach their ends.
Inputs may be any that keep to these rules, and one draw needn't show every extreme that they name: `images`: each row is a float embedding whose entries are not all zero. `texts`: each row is a float embedding of order one. `matches`: a permutation of the 2048 text indices.
All inputs are finite; a program needn't handle non-finite values.
Results may differ from the reference program's by a relative error of at most 0.0015.
The reference program's roundings to bfloat16 on the way (of `weights`) count: a program that leaves them out, or rounds other values in their place, can miss the bound.
Values may be sent and summed in bfloat16 or wider, within the bound.
A program may use at most 128 MiB of HBM per device.

```python
import math
import jax
import jax.numpy as jnp
from jax import lax

D = 1024
PAIRS = 2048


def pair_embeddings(key):
    base = jax.random.fold_in(key, 7)
    key_image, key_text = jax.random.split(base, 2)
    images = jax.random.normal(key_image, (PAIRS, D), jnp.float32)
    texts = jax.random.normal(key_text, (PAIRS, D), jnp.float32)
    return (images, texts)


def draw_images(key, part):
    return pair_embeddings(key)[0].astype(jnp.bfloat16)


def draw_texts(key, part):
    return pair_embeddings(key)[1].astype(jnp.bfloat16)


def setup_inputs(seed: int = 0) -> dict:
    key_of = jax.random.split(jax.random.key(seed), 5)
    images = draw_images(jax.random.fold_in(key_of[4], 71), 0)
    texts = draw_texts(jax.random.fold_in(key_of[4], 71), 0)
    matches = jax.random.permutation(key_of[2], PAIRS).astype(jnp.int32)
    logit_scale = jnp.clip(jnp.exp(jax.random.uniform(key_of[3], (), jnp.float32, math.log(20.0), math.log(400.0))), 20.0, 400.0)
    return {"images": images, "texts": texts, "matches": matches, "logit_scale": logit_scale}


EPSILON = 1e-06

def unit_rows(values):
    wide = values.astype(jnp.float32)
    norms = jnp.sqrt(lax.optimization_barrier(jnp.sum(wide * wide, axis=1, keepdims=True)) + EPSILON)
    return (wide / norms, norms)

def back_unit(unit, norms, grad):
    inner = lax.optimization_barrier(jnp.sum(unit * grad, axis=1, keepdims=True))
    return (grad - unit * inner) / norms

def reference(images, texts, matches, logit_scale):
    image_unit, image_norm = unit_rows(images)
    text_unit, text_norm = unit_rows(texts)
    image_low = image_unit.astype(jnp.bfloat16)
    text_low = text_unit.astype(jnp.bfloat16)
    scale = logit_scale.astype(jnp.float32)
    total = images.shape[0]
    block = math.gcd(total, 512)
    count = total // block
    image_blocks = image_low.reshape(count, block, image_low.shape[1])
    match_blocks = matches.reshape(count, block)
    columns = jnp.arange(total, dtype=jnp.int32)

    def forward(carry, item):
        col_max, col_sum, matched = carry
        rows, picks = item
        scores = scale * jnp.dot(rows, text_low.T, preferred_element_type=jnp.float32)
        row_max = lax.optimization_barrier(jnp.max(scores, axis=1))
        row_lse = row_max + jnp.log(lax.optimization_barrier(jnp.sum(jnp.exp(scores - row_max[:, None]), axis=1)))
        top = jnp.maximum(col_max, lax.optimization_barrier(jnp.max(scores, axis=0)))
        col_sum = col_sum * jnp.exp(col_max - top) + lax.optimization_barrier(jnp.sum(jnp.exp(scores - top[None, :]), axis=0))
        mask = picks[:, None] == columns[None, :]
        matched = matched + jnp.sum(jnp.where(mask, scores, jnp.float32(0.0)))
        return ((top, col_sum, matched), row_lse)
    start = (jnp.full((total,), -jnp.inf, jnp.float32), jnp.zeros((total,), jnp.float32), jnp.float32(0.0))
    (col_max, col_sum, matched), row_lse = lax.scan(forward, start, (image_blocks, match_blocks))
    col_lse = col_max + jnp.log(col_sum)
    row_lse = row_lse.reshape(total)
    loss = (jnp.sum(row_lse) + jnp.sum(col_lse)) / (2.0 * total) - matched / total

    def backward(text_acc, item):
        rows, picks, lse_rows = item
        scores = scale * jnp.dot(rows, text_low.T, preferred_element_type=jnp.float32)
        mask = (picks[:, None] == columns[None, :]).astype(jnp.float32)
        weights = 0.5 * jnp.exp(scores - lse_rows[:, None]) + 0.5 * jnp.exp(scores - col_lse[None, :]) - mask
        weights = (scale * weights).astype(jnp.bfloat16)
        image_part = jnp.dot(weights, text_low, preferred_element_type=jnp.float32)
        text_acc = text_acc + lax.dot_general(weights, rows, (((0,), (0,)), ((), ())), preferred_element_type=jnp.float32)
        return (text_acc, image_part)
    text_zero = jnp.zeros(text_low.shape, jnp.float32)
    text_unit_grad, image_parts = lax.scan(backward, text_zero, (image_blocks, match_blocks, row_lse.reshape(count, block)))
    image_unit_grad = image_parts.reshape(total, image_low.shape[1])
    image_grad = back_unit(image_unit, image_norm, image_unit_grad)
    text_grad = back_unit(text_unit, text_norm, text_unit_grad)
    return (loss, image_grad, text_grad)
```

```python
import functools

import jax
import jax.numpy as jnp
from jax import lax
from jax.experimental import pallas as pl
from jax.experimental.pallas import tpu as pltpu
from jax.sharding import PartitionSpec as P

EPSILON = 1e-06
MESH = pl.DeviceIdType.MESH


def merged(value, axis, join):
    pieces = jax.tree.map(lambda part: lax.all_gather(part, axis), value)
    head = jax.tree.map(lambda part: part[0], pieces)
    tail = jax.tree.map(lambda part: part[1:], pieces)
    running, _ = lax.scan(lambda running, piece: (join(running, piece), None), head, tail)
    return running


def unit_rows(values):
    wide = values.astype(jnp.float32)
    norms = jnp.sqrt(jnp.sum(wide * wide, axis=1, keepdims=True) + EPSILON)
    return (wide / norms, norms)


def back_unit(unit, norms, grad):
    inner = jnp.sum(unit * grad, axis=1, keepdims=True)
    return (grad - unit * inner) / norms


def combine_stats(first, second):
    top = jnp.maximum(first[0], second[0])
    return (top, first[1] * jnp.exp(first[0] - top) + second[1] * jnp.exp(second[0] - top))


def on_device(images, texts, matches, logit_scale):
    per_dev = images.shape[0]
    n_row = lax.axis_size("row")
    n_col = lax.axis_size("col")
    total = per_dev * n_row * n_col
    col_pos = lax.axis_index("col")
    row_pos = lax.axis_index("row")
    image_unit, image_norm = unit_rows(images)
    text_unit, text_norm = unit_rows(texts)
    image_low = image_unit.astype(jnp.bfloat16)
    text_low = text_unit.astype(jnp.bfloat16)
    image_rows = lax.all_gather(image_low, "col", axis=0, tiled=True)
    half = 0
    stride = 1
    n_img = image_rows.shape[0]

    def scores_of(piece):
        return logit_scale * lax.dot_general(
            piece, image_rows, (((1,), (1,)), ((), ())), preferred_element_type=jnp.float32
        )

    def match_mask(count):
        place = jnp.arange(count, dtype=jnp.int32)
        owner = place // per_dev * stride + half
        text_ids = owner * (n_col * per_dev) + col_pos * per_dev + place % per_dev
        return text_ids[:, None] == matches[None, :]

    piece = lax.all_gather(text_low, "row", axis=0, tiled=True)
    row_max = jnp.full((n_img,), -jnp.inf, jnp.float32)
    row_sum = jnp.zeros((n_img,), jnp.float32)
    scores = scores_of(piece)
    top = jnp.max(scores, axis=0)
    row_sum = row_sum * jnp.exp(row_max - top) + jnp.sum(jnp.exp(scores - top[None, :]), axis=0)
    piece_max = jnp.max(scores, axis=1)
    piece_sum = jnp.sum(jnp.exp(scores - piece_max[:, None]), axis=1)
    col_max = piece_max
    col_sum = piece_sum
    mask = match_mask(piece.shape[0])
    matched = jnp.sum(jnp.where(mask, scores, jnp.float32(0.0)))
    stats = (top, row_sum, col_max, col_sum, matched)
    row_max, row_sum, col_max, col_sum, matched = stats
    row_max, row_sum = merged((row_max, row_sum), "col", combine_stats)
    slot_max = col_max
    slot_sum = col_sum
    slot_max, slot_sum = merged((slot_max, slot_sum), "row", combine_stats)
    col_max = slot_max
    col_sum = slot_sum
    row_lse = row_max + jnp.log(row_sum)
    col_lse = col_max + jnp.log(col_sum)
    own_rows = jnp.sum(
        lax.dynamic_slice_in_dim(row_lse, (half * n_col + col_pos) * per_dev, per_dev, 0)
    )
    own_cols = jnp.sum(lax.dynamic_slice_in_dim(col_lse, row_pos // stride * per_dev, per_dev, 0))
    share = (own_rows + own_cols) / (2.0 * total) - matched / total
    loss = lax.psum(share, ("row", "col"))
    piece = lax.all_gather(text_low, "row", axis=0, tiled=True)
    count = piece.shape[0]
    scores = scores_of(piece)
    mask = match_mask(count).astype(jnp.float32)
    weights = (
        0.5 * jnp.exp(scores - row_lse[None, :]) + 0.5 * jnp.exp(scores - col_lse[:, None]) - mask
    )
    weights = (logit_scale * weights).astype(jnp.bfloat16)
    image_acc = lax.dot_general(
        weights, piece, (((0,), (0,)), ((), ())), preferred_element_type=jnp.float32
    )
    text_piece = jnp.dot(weights, image_rows, preferred_element_type=jnp.float32)
    text_acc = text_piece
    image_acc, text_acc = (image_acc, text_acc)
    image_unit_grad = lax.psum_scatter(image_acc, "col", scatter_dimension=0, tiled=True)
    text_unit_grad = lax.psum_scatter(text_acc, "row", scatter_dimension=0, tiled=True)
    image_grad = back_unit(image_unit, image_norm, image_unit_grad)
    text_grad = back_unit(text_unit, text_norm, text_unit_grad)
    return (loss, image_grad, text_grad)


def fused_kernel(
    n_row, n_col, img_ref, txt_ref, match_ref, scale_ref, loss_ref, gimg_ref, gtxt_ref,
    raw, low, own, sc, ex, wbuf, stat, tile, lsem, ssem, rsem,
):
    per = img_ref.shape[0]
    n_dev = n_row * n_col
    total = per * n_dev
    units = raw.shape[1]
    width = 4 * per
    pair = 2 * per
    row = lax.axis_index("row")
    x = lax.axis_index("col")
    z, y, c = row // 4, (row // 2) % 2, row % 2
    me = row * n_col + x
    scale = scale_ref[0, 0]

    def place(zz, yy, cc, xx):
        return ((zz * 4 + yy * 2 + cc), xx)

    barrier = pltpu.get_barrier_semaphore()
    peers = [(me + k) % n_dev for k in range(1, n_dev)]
    peers = [(p // n_col, p % n_col) for p in peers]
    for peer in peers:
        pl.semaphore_signal(barrier, inc=1, device_id=peer, device_id_type=MESH)

    inputs = (img_ref, txt_ref)
    kept = [
        pltpu.make_async_copy(inputs[a], raw.at[a, z * 2 + y, c * 2 + x], lsem.at[a])
        for a in range(2)
    ]
    for copy in kept:
        copy.start()
    for a in range(2):
        wide = inputs[a][...].astype(jnp.float32)
        norm = jnp.sqrt(jnp.sum(wide * wide, axis=1, keepdims=True) + EPSILON)
        own[a] = (wide * (1.0 / norm)).astype(jnp.bfloat16)
    for copy in kept:
        copy.wait()
    pl.semaphore_wait(barrier, n_dev - 1)

    copies = []

    def send(src, dst, target):
        k = len(copies)
        copy = pltpu.make_async_remote_copy(
            src_ref=src, dst_ref=dst, send_sem=ssem.at[k], recv_sem=rsem.at[k],
            device_id=target, device_id_type=MESH,
        )
        copy.start()
        copies.append(copy)
        return copy

    def move(a, zz, yy, xx, target):
        ref = raw.at[a, zz * 2 + yy, c * 2 + xx]
        return send(ref, ref, target)

    to_x, to_y = place(z, y, c, 1 - x), place(z, 1 - y, c, x)
    sibling = place(z, y, 1 - c, x)

    def share(zz, yy, xx):
        ref = raw.at[:, zz * 2 + yy, c * 2 + xx]
        return send(ref, ref, sibling)

    def zmate(k):
        low_bit, high_bit = z % 2, z // 2
        if k & 1:
            low_bit = 1 - low_bit
        if k & 2:
            high_bit = 1 - high_bit
        return high_bit * 2 + low_bit

    zs = [zmate(k) for k in range(4)]

    def process(zz, yy):
        unit = zz * 2 + yy
        for a in range(2):
            @pl.loop(0, 4)
            def _(b):
                wide = raw[a, unit, b].astype(jnp.float32)
                norm = jnp.sqrt(jnp.sum(wide * wide, axis=1, keepdims=True) + EPSILON)
                rows = pl.ds(pl.multiple_of(unit * width + b * per, per), per)
                low[a, rows, :] = (wide * (1.0 / norm)).astype(jnp.bfloat16)

            rows = pl.ds(pl.multiple_of(unit * width, width), width)
            sc[a, unit] = scale * lax.dot_general(
                own[1 - a], low[a, rows, :], (((1,), (1,)), ((), ())),
                preferred_element_type=jnp.float32,
            )

    lines = [None]
    first, second, third, shares = {}, {}, {}, {}

    def stage1(k):
        if k:
            for copy in lines[k]:
                copy.wait_recv()
        ax = move(0, zs[k], y, x, to_x)
        by = move(1, zs[k], y, x, to_y)
        bx = move(1, zs[k], y, x, to_x)
        ay = move(0, zs[k], y, x, to_y)
        first[k] = (ax, by)
        second[k] = (bx, ay)
        shares[k] = [share(zs[k], y, x)]

    def stage2(k):
        ax, by = first[k]
        ax.wait_recv()
        ady = move(0, zs[k], y, 1 - x, to_y)
        by.wait_recv()
        bdx = move(1, zs[k], 1 - y, x, to_x)
        third[k] = (ady, bdx)

    def stage3(k):
        bx, ay = second[k]
        bx.wait_recv()
        shares[k].append(share(zs[k], y, 1 - x))
        ay.wait_recv()
        shares[k].append(share(zs[k], 1 - y, x))

    def stage4(k):
        for copy in third[k]:
            copy.wait_recv()
        shares[k].append(share(zs[k], 1 - y, 1 - x))

    stage1(0)
    for k in range(1, 4):
        lines.append([move(a, z, y, x, place(zs[k], y, c, x)) for a in range(2)])
    stage2(0)
    for k in range(4):
        if k + 1 < 4:
            stage1(k + 1)
        stage3(k)
        shares[k][0].wait_recv()
        shares[k][1].wait_recv()
        process(zs[k], y)
        stage4(k)
        if k + 1 < 4:
            stage2(k + 1)
        shares[k][2].wait_recv()
        shares[k][3].wait_recv()
        process(zs[k], 1 - y)

    lane = lax.broadcasted_iota(jnp.int32, (per, pair), 1)
    sub = lax.broadcasted_iota(jnp.int32, (per, pair), 0)
    eye = lane == sub + x * per
    match_row = match_ref[...].astype(jnp.float32)
    match_own = jnp.sum(jnp.where(eye, match_row, 0.0), axis=1, keepdims=True)
    lses, sums = [None, None], [None, None]
    for a in range(2):
        top = jnp.max(sc[a, 0], axis=1, keepdims=True)
        for u in range(1, units):
            top = jnp.maximum(top, jnp.max(sc[a, u], axis=1, keepdims=True))
        acc = jnp.zeros((per, width), jnp.float32)
        for u in range(units):
            e = jnp.exp(sc[a, u] - top)
            ex[a, u] = e
            acc = acc + e
        sums[a] = jnp.sum(acc, axis=1, keepdims=True)
        lses[a] = top + jnp.log(sums[a])
    unit_lane = lax.broadcasted_iota(jnp.int32, (per, width), 1).astype(jnp.float32)
    hit = jnp.zeros((per, width), jnp.float32)
    for u in range(units):
        hit = hit + jnp.where(unit_lane + float(u * width) == match_own, sc[1, u], 0.0)
    matched = jnp.sum(jnp.sum(hit, axis=1, keepdims=True), axis=0, keepdims=True)

    def as_lanes(column):
        return jnp.sum(jnp.where(eye, column, 0.0), axis=0, keepdims=True)

    here = lax.broadcasted_iota(jnp.int32, (1, pair), 1)
    inside = (here >= x * per) & (here < (x + 1) * per)
    tile[0:1, :] = as_lanes(lses[1])
    tile[1:2, :] = as_lanes(lses[0])
    tile[2:3, :] = jnp.where(inside, match_row, 0.0)
    tile[3:4, :] = jnp.where(here == 0, matched, 0.0)
    tile[4:8, :] = jnp.zeros((4, pair), jnp.float32)
    stat[me] = tile[...]
    news = [send(tile, stat.at[me], peer) for peer in peers]

    for a in range(2):
        half = 0.5 / sums[a]
        for u in range(units):
            part = ex[a, u] * half
            if a == 1:
                part = part - jnp.where(unit_lane + float(u * width) == match_own, 1.0, 0.0)
            ex[a, u] = part

    for copy in news:
        copy.wait_recv()
    blocks = [stat[2 * k] + stat[2 * k + 1] for k in range(n_dev // 2)]
    everyone = blocks[0]
    for block in blocks[1:]:
        everyone = everyone + block
    rows8 = lax.broadcasted_iota(jnp.int32, everyone.shape, 0)
    factor = jnp.where(rows8 < 2, 0.5 / total, jnp.where(rows8 == 3, -1.0 / total, 0.0))
    loss_ref[...] = jnp.sum(
        jnp.sum(everyone * factor, axis=1, keepdims=True), axis=0, keepdims=True
    )
    text_id = (
        lax.broadcasted_iota(jnp.int32, (per, 1), 0) + me * per
    ).astype(jnp.float32)
    for a in (1, 0):
        for u in range(units):
            wide = jnp.concatenate([blocks[2 * u], blocks[2 * u + 1]], axis=1)
            other = wide[1:2, :] if a == 1 else wide[0:1, :]
            value = ex[a, u] + 0.5 * jnp.exp(sc[a, u] - other)
            if a == 0:
                value = value - jnp.where(wide[2:3, :] == text_id, 1.0, 0.0)
            wbuf[a, :, u * width : (u + 1) * width] = (scale * value).astype(jnp.bfloat16)
        grad = jnp.dot(wbuf[a], low[a], preferred_element_type=jnp.float32)
        source, out = (img_ref, gimg_ref) if a == 1 else (txt_ref, gtxt_ref)
        wide = source[...].astype(jnp.float32)
        norm = jnp.sqrt(jnp.sum(wide * wide, axis=1, keepdims=True) + EPSILON)
        inv = 1.0 / norm
        unit = wide * inv
        inner = jnp.sum(unit * grad, axis=1, keepdims=True)
        out[...] = (grad - unit * inner) * inv
    for copy in copies:
        copy.wait_send()


def fused(n_row, n_col, images, texts, matches, logit_scale):
    per, d = images.shape
    n_dev = n_row * n_col
    units = n_dev // 4
    n_sem = 6 + 10 * 4 + n_dev - 1
    vmem = pl.BlockSpec(memory_space=pltpu.VMEM)
    loss, image_grad, text_grad = pl.pallas_call(
        functools.partial(fused_kernel, n_row, n_col),
        out_shape=(
            jax.ShapeDtypeStruct((1, 1), jnp.float32),
            jax.ShapeDtypeStruct((per, d), jnp.float32),
            jax.ShapeDtypeStruct((per, d), jnp.float32),
        ),
        in_specs=[vmem, vmem, vmem, pl.BlockSpec(memory_space=pltpu.SMEM)],
        out_specs=(vmem, vmem, vmem),
        scratch_shapes=[
            pltpu.VMEM((2, units, 4, per, d), jnp.bfloat16),
            pltpu.VMEM((2, units * 4 * per, d), jnp.bfloat16),
            pltpu.VMEM((2, per, d), jnp.bfloat16),
            pltpu.VMEM((2, units, per, 4 * per), jnp.float32),
            pltpu.VMEM((2, units, per, 4 * per), jnp.float32),
            pltpu.VMEM((2, per, units * 4 * per), jnp.bfloat16),
            pltpu.VMEM((n_dev, 8, 2 * per), jnp.float32),
            pltpu.VMEM((8, 2 * per), jnp.float32),
            pltpu.SemaphoreType.DMA((2,)),
            pltpu.SemaphoreType.DMA((n_sem,)),
            pltpu.SemaphoreType.DMA((n_sem,)),
        ],
        compiler_params=pltpu.CompilerParams(
            collective_id=0, has_side_effects=True, vmem_limit_bytes=56 * 1024 * 1024
        ),
    )(images, texts, matches.reshape(1, -1), logit_scale.reshape(1, 1))
    return loss.reshape(()), image_grad, text_grad


def solution(mesh):
    placed = (P(("row", "col"), None), P(("row", "col"), None), P("row"), P())
    n_row, n_col = mesh.shape["row"], mesh.shape["col"]

    def body(images, texts, matches, logit_scale):
        if n_col == 2 and n_row == 16 and matches.shape[0] == 128:
            return fused(n_row, n_col, images, texts, matches, logit_scale)
        return on_device(images, texts, matches, logit_scale)

    return jax.shard_map(
        body,
        mesh=mesh,
        in_specs=placed,
        out_specs=(P(), P(("row", "col"), None), P(("row", "col"), None)),
        check_vma=False,
    )
```

```python
import functools

import jax
import jax.numpy as jnp
from jax import lax
from jax.experimental import pallas as pl
from jax.experimental.pallas import tpu as pltpu
from jax.sharding import PartitionSpec as P

EPSILON = 1e-06
MESH = pl.DeviceIdType.MESH


def merged(value, axis, join):
    pieces = jax.tree.map(lambda part: lax.all_gather(part, axis), value)
    head = jax.tree.map(lambda part: part[0], pieces)
    tail = jax.tree.map(lambda part: part[1:], pieces)
    running, _ = lax.scan(lambda running, piece: (join(running, piece), None), head, tail)
    return running


def unit_rows(values):
    wide = values.astype(jnp.float32)
    norms = jnp.sqrt(jnp.sum(wide * wide, axis=1, keepdims=True) + EPSILON)
    return (wide / norms, norms)


def back_unit(unit, norms, grad):
    inner = jnp.sum(unit * grad, axis=1, keepdims=True)
    return (grad - unit * inner) / norms


def combine_stats(first, second):
    top = jnp.maximum(first[0], second[0])
    return (top, first[1] * jnp.exp(first[0] - top) + second[1] * jnp.exp(second[0] - top))


def on_device(images, texts, matches, logit_scale):
    per_dev = images.shape[0]
    n_row = lax.axis_size("row")
    n_col = lax.axis_size("col")
    total = per_dev * n_row * n_col
    col_pos = lax.axis_index("col")
    row_pos = lax.axis_index("row")
    image_unit, image_norm = unit_rows(images)
    text_unit, text_norm = unit_rows(texts)
    image_low = image_unit.astype(jnp.bfloat16)
    text_low = text_unit.astype(jnp.bfloat16)
    image_rows = lax.all_gather(image_low, "col", axis=0, tiled=True)
    half = 0
    stride = 1
    n_img = image_rows.shape[0]

    def scores_of(piece):
        return logit_scale * lax.dot_general(
            piece, image_rows, (((1,), (1,)), ((), ())), preferred_element_type=jnp.float32
        )

    def match_mask(count):
        place = jnp.arange(count, dtype=jnp.int32)
        owner = place // per_dev * stride + half
        text_ids = owner * (n_col * per_dev) + col_pos * per_dev + place % per_dev
        return text_ids[:, None] == matches[None, :]

    piece = lax.all_gather(text_low, "row", axis=0, tiled=True)
    row_max = jnp.full((n_img,), -jnp.inf, jnp.float32)
    row_sum = jnp.zeros((n_img,), jnp.float32)
    scores = scores_of(piece)
    top = jnp.max(scores, axis=0)
    row_sum = row_sum * jnp.exp(row_max - top) + jnp.sum(jnp.exp(scores - top[None, :]), axis=0)
    piece_max = jnp.max(scores, axis=1)
    piece_sum = jnp.sum(jnp.exp(scores - piece_max[:, None]), axis=1)
    col_max = piece_max
    col_sum = piece_sum
    mask = match_mask(piece.shape[0])
    matched = jnp.sum(jnp.where(mask, scores, jnp.float32(0.0)))
    stats = (top, row_sum, col_max, col_sum, matched)
    row_max, row_sum, col_max, col_sum, matched = stats
    row_max, row_sum = merged((row_max, row_sum), "col", combine_stats)
    slot_max = col_max
    slot_sum = col_sum
    slot_max, slot_sum = merged((slot_max, slot_sum), "row", combine_stats)
    col_max = slot_max
    col_sum = slot_sum
    row_lse = row_max + jnp.log(row_sum)
    col_lse = col_max + jnp.log(col_sum)
    own_rows = jnp.sum(
        lax.dynamic_slice_in_dim(row_lse, (half * n_col + col_pos) * per_dev, per_dev, 0)
    )
    own_cols = jnp.sum(lax.dynamic_slice_in_dim(col_lse, row_pos // stride * per_dev, per_dev, 0))
    share = (own_rows + own_cols) / (2.0 * total) - matched / total
    loss = lax.psum(share, ("row", "col"))
    piece = lax.all_gather(text_low, "row", axis=0, tiled=True)
    count = piece.shape[0]
    scores = scores_of(piece)
    mask = match_mask(count).astype(jnp.float32)
    weights = (
        0.5 * jnp.exp(scores - row_lse[None, :]) + 0.5 * jnp.exp(scores - col_lse[:, None]) - mask
    )
    weights = (logit_scale * weights).astype(jnp.bfloat16)
    image_acc = lax.dot_general(
        weights, piece, (((0,), (0,)), ((), ())), preferred_element_type=jnp.float32
    )
    text_piece = jnp.dot(weights, image_rows, preferred_element_type=jnp.float32)
    text_acc = text_piece
    image_acc, text_acc = (image_acc, text_acc)
    image_unit_grad = lax.psum_scatter(image_acc, "col", scatter_dimension=0, tiled=True)
    text_unit_grad = lax.psum_scatter(text_acc, "row", scatter_dimension=0, tiled=True)
    image_grad = back_unit(image_unit, image_norm, image_unit_grad)
    text_grad = back_unit(text_unit, text_norm, text_unit_grad)
    return (loss, image_grad, text_grad)


def fused_kernel(
    n_row, n_col, img_ref, txt_ref, match_ref, scale_ref, loss_ref, gimg_ref, gtxt_ref,
    raw, low, own, sc, ex, wbuf, stat, tile, lsem, ssem, rsem,
):
    per = img_ref.shape[0]
    n_dev = n_row * n_col
    total = per * n_dev
    units = raw.shape[1]
    width = 4 * per
    pair = 2 * per
    row = lax.axis_index("row")
    x = lax.axis_index("col")
    z, y, c = row // 4, (row // 2) % 2, row % 2
    me = row * n_col + x
    scale = scale_ref[0, 0]

    def place(zz, yy, cc, xx):
        return ((zz * 4 + yy * 2 + cc), xx)

    barrier = pltpu.get_barrier_semaphore()
    peers = [(me + k) % n_dev for k in range(1, n_dev)]
    peers = [(p // n_col, p % n_col) for p in peers]
    greet = [(row,1-x),(z*4+(1-y)*2+c,x),(z*4+y*2+1-c,x)]+[(((z+k)%4)*4+y*2+c,x) for k in (1,2,3)]
    for peer in greet:
        pl.semaphore_signal(barrier, inc=1, device_id=peer, device_id_type=MESH)

    inputs = (img_ref, txt_ref)
    kept = [
        pltpu.make_async_copy(inputs[a], raw.at[a, z * 2 + y, c * 2 + x], lsem.at[a])
        for a in range(2)
    ]
    for copy in kept:
        copy.start()
    for a in range(2):
        wide = inputs[a][...].astype(jnp.float32)
        norm = jnp.sqrt(jnp.sum(wide * wide, axis=1, keepdims=True) + EPSILON)
        own[a] = (wide * (1.0 / norm)).astype(jnp.bfloat16)
    for copy in kept:
        copy.wait()
    pl.semaphore_wait(barrier, len(greet))

    copies = []

    def send(src, dst, target):
        k = len(copies)
        copy = pltpu.make_async_remote_copy(
            src_ref=src, dst_ref=dst, send_sem=ssem.at[k], recv_sem=rsem.at[k],
            device_id=target, device_id_type=MESH,
        )
        copy.start()
        copies.append(copy)
        return copy

    def move(a, zz, yy, xx, target):
        ref = raw.at[a, zz * 2 + yy, c * 2 + xx]
        return send(ref, ref, target)

    to_x, to_y = place(z, y, c, 1 - x), place(z, 1 - y, c, x)
    sibling = place(z, y, 1 - c, x)

    def share(zz, yy, xx):
        ref = raw.at[:, zz * 2 + yy, c * 2 + xx]
        return send(ref, ref, sibling)

    def zmate(k):
        low_bit, high_bit = z % 2, z // 2
        if k & 1:
            low_bit = 1 - low_bit
        if k & 2:
            high_bit = 1 - high_bit
        return high_bit * 2 + low_bit

    zs = [zmate(k) for k in range(4)]

    def process(zz, yy):
        unit = zz * 2 + yy
        for a in range(2):
            @pl.loop(0, 4)
            def _(b):
                wide = raw[a, unit, b].astype(jnp.float32)
                norm = jnp.sqrt(jnp.sum(wide * wide, axis=1, keepdims=True) + EPSILON)
                rows = pl.ds(pl.multiple_of(unit * width + b * per, per), per)
                low[a, rows, :] = (wide * (1.0 / norm)).astype(jnp.bfloat16)

            rows = pl.ds(pl.multiple_of(unit * width, width), width)
            sc[a, unit] = scale * lax.dot_general(
                own[1 - a], low[a, rows, :], (((1,), (1,)), ((), ())),
                preferred_element_type=jnp.float32,
            )

    lines = [None]
    first, second, third, shares = {}, {}, {}, {}

    def stage1(k):
        if k:
            for copy in lines[k]:
                copy.wait_recv()
        ax = move(0, zs[k], y, x, to_x)
        by = move(1, zs[k], y, x, to_y)
        bx = move(1, zs[k], y, x, to_x)
        ay = move(0, zs[k], y, x, to_y)
        first[k] = (ax, by)
        second[k] = (bx, ay)
        shares[k] = [share(zs[k], y, x)]

    def stage2(k):
        ax, by = first[k]
        ax.wait_recv()
        ady = move(0, zs[k], y, 1 - x, to_y)
        by.wait_recv()
        bdx = move(1, zs[k], 1 - y, x, to_x)
        third[k] = (ady, bdx)

    def stage3(k):
        bx, ay = second[k]
        bx.wait_recv()
        shares[k].append(share(zs[k], y, 1 - x))
        ay.wait_recv()
        shares[k].append(share(zs[k], 1 - y, x))

    def stage4(k):
        for copy in third[k]:
            copy.wait_recv()
        shares[k].append(share(zs[k], 1 - y, 1 - x))

    stage1(0)
    for k in range(1, 4):
        lines.append([move(a, z, y, x, place(zs[k], y, c, x)) for a in range(2)])
    stage2(0)
    for k in range(4):
        if k + 1 < 4:
            stage1(k + 1)
        stage3(k)
        shares[k][0].wait_recv()
        shares[k][1].wait_recv()
        process(zs[k], y)
        stage4(k)
        if k + 1 < 4:
            stage2(k + 1)
        shares[k][2].wait_recv()
        shares[k][3].wait_recv()
        process(zs[k], 1 - y)

    lane = lax.broadcasted_iota(jnp.int32, (per, pair), 1)
    sub = lax.broadcasted_iota(jnp.int32, (per, pair), 0)
    eye = lane == sub + x * per
    match_row = match_ref[...].astype(jnp.float32)
    match_own = jnp.sum(jnp.where(eye, match_row, 0.0), axis=1, keepdims=True)
    lses, sums = [None, None], [None, None]
    for a in range(2):
        top = jnp.max(sc[a, 0], axis=1, keepdims=True)
        for u in range(1, units):
            top = jnp.maximum(top, jnp.max(sc[a, u], axis=1, keepdims=True))
        acc = jnp.zeros((per, width), jnp.float32)
        for u in range(units):
            e = jnp.exp(sc[a, u] - top)
            ex[a, u] = e
            acc = acc + e
        sums[a] = jnp.sum(acc, axis=1, keepdims=True)
        lses[a] = top + jnp.log(sums[a])
    unit_lane = lax.broadcasted_iota(jnp.int32, (per, width), 1).astype(jnp.float32)
    hit = jnp.zeros((per, width), jnp.float32)
    for u in range(units):
        hit = hit + jnp.where(unit_lane + float(u * width) == match_own, sc[1, u], 0.0)
    matched = jnp.sum(jnp.sum(hit, axis=1, keepdims=True), axis=0, keepdims=True)

    def as_lanes(column):
        return jnp.sum(jnp.where(eye, column, 0.0), axis=0, keepdims=True)

    here = lax.broadcasted_iota(jnp.int32, (1, pair), 1)
    inside = (here >= x * per) & (here < (x + 1) * per)
    tile[0:1, :] = as_lanes(lses[1])
    tile[1:2, :] = as_lanes(lses[0])
    tile[2:3, :] = jnp.where(inside, match_row, 0.0)
    tile[3:4, :] = jnp.where(here == 0, matched, 0.0)
    tile[4:8, :] = jnp.zeros((4, pair), jnp.float32)
    stat[me] = tile[...]
    news = [send(tile, stat.at[me], peer) for peer in peers]

    for a in range(2):
        half = 0.5 / sums[a]
        for u in range(units):
            part = ex[a, u] * half
            if a == 1:
                part = part - jnp.where(unit_lane + float(u * width) == match_own, 1.0, 0.0)
            ex[a, u] = part

    for copy in news:
        copy.wait_recv()
    blocks = [stat[2 * k] + stat[2 * k + 1] for k in range(n_dev // 2)]
    everyone = blocks[0]
    for block in blocks[1:]:
        everyone = everyone + block
    rows8 = lax.broadcasted_iota(jnp.int32, everyone.shape, 0)
    factor = jnp.where(rows8 < 2, 0.5 / total, jnp.where(rows8 == 3, -1.0 / total, 0.0))
    loss_ref[...] = jnp.sum(
        jnp.sum(everyone * factor, axis=1, keepdims=True), axis=0, keepdims=True
    )
    text_id = (
        lax.broadcasted_iota(jnp.int32, (per, 1), 0) + me * per
    ).astype(jnp.float32)
    for a in (1, 0):
        for u in range(units):
            wide = jnp.concatenate([blocks[2 * u], blocks[2 * u + 1]], axis=1)
            other = wide[1:2, :] if a == 1 else wide[0:1, :]
            value = ex[a, u] + 0.5 * jnp.exp(sc[a, u] - other)
            if a == 0:
                value = value - jnp.where(wide[2:3, :] == text_id, 1.0, 0.0)
            wbuf[a, :, u * width : (u + 1) * width] = (scale * value).astype(jnp.bfloat16)
        grad = jnp.dot(wbuf[a], low[a], preferred_element_type=jnp.float32)
        source, out = (img_ref, gimg_ref) if a == 1 else (txt_ref, gtxt_ref)
        wide = source[...].astype(jnp.float32)
        norm = jnp.sqrt(jnp.sum(wide * wide, axis=1, keepdims=True) + EPSILON)
        inv = 1.0 / norm
        unit = wide * inv
        inner = jnp.sum(unit * grad, axis=1, keepdims=True)
        out[...] = (grad - unit * inner) * inv
    for copy in copies:
        copy.wait_send()


def fused(n_row, n_col, images, texts, matches, logit_scale):
    per, d = images.shape
    n_dev = n_row * n_col
    units = n_dev // 4
    n_sem = 6 + 10 * 4 + n_dev - 1
    vmem = pl.BlockSpec(memory_space=pltpu.VMEM)
    loss, image_grad, text_grad = pl.pallas_call(
        functools.partial(fused_kernel, n_row, n_col),
        out_shape=(
            jax.ShapeDtypeStruct((1, 1), jnp.float32),
            jax.ShapeDtypeStruct((per, d), jnp.float32),
            jax.ShapeDtypeStruct((per, d), jnp.float32),
        ),
        in_specs=[vmem, vmem, vmem, pl.BlockSpec(memory_space=pltpu.SMEM)],
        out_specs=(vmem, vmem, vmem),
        scratch_shapes=[
            pltpu.VMEM((2, units, 4, per, d), jnp.bfloat16),
            pltpu.VMEM((2, units * 4 * per, d), jnp.bfloat16),
            pltpu.VMEM((2, per, d), jnp.bfloat16),
            pltpu.VMEM((2, units, per, 4 * per), jnp.float32),
            pltpu.VMEM((2, units, per, 4 * per), jnp.float32),
            pltpu.VMEM((2, per, units * 4 * per), jnp.bfloat16),
            pltpu.VMEM((n_dev, 8, 2 * per), jnp.float32),
            pltpu.VMEM((8, 2 * per), jnp.float32),
            pltpu.SemaphoreType.DMA((2,)),
            pltpu.SemaphoreType.DMA((n_sem,)),
            pltpu.SemaphoreType.DMA((n_sem,)),
        ],
        compiler_params=pltpu.CompilerParams(
            collective_id=0, has_side_effects=True, vmem_limit_bytes=56 * 1024 * 1024
        ),
    )(images, texts, matches.reshape(1, -1), logit_scale.reshape(1, 1))
    return loss.reshape(()), image_grad, text_grad


def solution(mesh):
    placed = (P(("row", "col"), None), P(("row", "col"), None), P("row"), P())
    n_row, n_col = mesh.shape["row"], mesh.shape["col"]

    def body(images, texts, matches, logit_scale):
        if n_col == 2 and n_row == 16 and matches.shape[0] == 128:
            return fused(n_row, n_col, images, texts, matches, logit_scale)
        return on_device(images, texts, matches, logit_scale)

    return jax.shard_map(
        body,
        mesh=mesh,
        in_specs=placed,
        out_specs=(P(), P(("row", "col"), None), P(("row", "col"), None)),
        check_vma=False,
    )
```

```python
import functools

import jax
import jax.numpy as jnp
from jax import lax
from jax.experimental import pallas as pl
from jax.experimental.pallas import tpu as pltpu
from jax.sharding import PartitionSpec as P

EPSILON = 1e-06
MESH = pl.DeviceIdType.MESH


def merged(value, axis, join):
    pieces = jax.tree.map(lambda part: lax.all_gather(part, axis), value)
    head = jax.tree.map(lambda part: part[0], pieces)
    tail = jax.tree.map(lambda part: part[1:], pieces)
    running, _ = lax.scan(lambda running, piece: (join(running, piece), None), head, tail)
    return running


def unit_rows(values):
    wide = values.astype(jnp.float32)
    norms = jnp.sqrt(jnp.sum(wide * wide, axis=1, keepdims=True) + EPSILON)
    return (wide / norms, norms)


def back_unit(unit, norms, grad):
    inner = jnp.sum(unit * grad, axis=1, keepdims=True)
    return (grad - unit * inner) / norms


def combine_stats(first, second):
    top = jnp.maximum(first[0], second[0])
    return (top, first[1] * jnp.exp(first[0] - top) + second[1] * jnp.exp(second[0] - top))


def on_device(images, texts, matches, logit_scale):
    per_dev = images.shape[0]
    n_row = lax.axis_size("row")
    n_col = lax.axis_size("col")
    total = per_dev * n_row * n_col
    col_pos = lax.axis_index("col")
    row_pos = lax.axis_index("row")
    image_unit, image_norm = unit_rows(images)
    text_unit, text_norm = unit_rows(texts)
    image_low = image_unit.astype(jnp.bfloat16)
    text_low = text_unit.astype(jnp.bfloat16)
    image_rows = lax.all_gather(image_low, "col", axis=0, tiled=True)
    half = 0
    stride = 1
    n_img = image_rows.shape[0]

    def scores_of(piece):
        return logit_scale * lax.dot_general(
            piece, image_rows, (((1,), (1,)), ((), ())), preferred_element_type=jnp.float32
        )

    def match_mask(count):
        place = jnp.arange(count, dtype=jnp.int32)
        owner = place // per_dev * stride + half
        text_ids = owner * (n_col * per_dev) + col_pos * per_dev + place % per_dev
        return text_ids[:, None] == matches[None, :]

    piece = lax.all_gather(text_low, "row", axis=0, tiled=True)
    row_max = jnp.full((n_img,), -jnp.inf, jnp.float32)
    row_sum = jnp.zeros((n_img,), jnp.float32)
    scores = scores_of(piece)
    top = jnp.max(scores, axis=0)
    row_sum = row_sum * jnp.exp(row_max - top) + jnp.sum(jnp.exp(scores - top[None, :]), axis=0)
    piece_max = jnp.max(scores, axis=1)
    piece_sum = jnp.sum(jnp.exp(scores - piece_max[:, None]), axis=1)
    col_max = piece_max
    col_sum = piece_sum
    mask = match_mask(piece.shape[0])
    matched = jnp.sum(jnp.where(mask, scores, jnp.float32(0.0)))
    stats = (top, row_sum, col_max, col_sum, matched)
    row_max, row_sum, col_max, col_sum, matched = stats
    row_max, row_sum = merged((row_max, row_sum), "col", combine_stats)
    slot_max = col_max
    slot_sum = col_sum
    slot_max, slot_sum = merged((slot_max, slot_sum), "row", combine_stats)
    col_max = slot_max
    col_sum = slot_sum
    row_lse = row_max + jnp.log(row_sum)
    col_lse = col_max + jnp.log(col_sum)
    own_rows = jnp.sum(
        lax.dynamic_slice_in_dim(row_lse, (half * n_col + col_pos) * per_dev, per_dev, 0)
    )
    own_cols = jnp.sum(lax.dynamic_slice_in_dim(col_lse, row_pos // stride * per_dev, per_dev, 0))
    share = (own_rows + own_cols) / (2.0 * total) - matched / total
    loss = lax.psum(share, ("row", "col"))
    piece = lax.all_gather(text_low, "row", axis=0, tiled=True)
    count = piece.shape[0]
    scores = scores_of(piece)
    mask = match_mask(count).astype(jnp.float32)
    weights = (
        0.5 * jnp.exp(scores - row_lse[None, :]) + 0.5 * jnp.exp(scores - col_lse[:, None]) - mask
    )
    weights = (logit_scale * weights).astype(jnp.bfloat16)
    image_acc = lax.dot_general(
        weights, piece, (((0,), (0,)), ((), ())), preferred_element_type=jnp.float32
    )
    text_piece = jnp.dot(weights, image_rows, preferred_element_type=jnp.float32)
    text_acc = text_piece
    image_acc, text_acc = (image_acc, text_acc)
    image_unit_grad = lax.psum_scatter(image_acc, "col", scatter_dimension=0, tiled=True)
    text_unit_grad = lax.psum_scatter(text_acc, "row", scatter_dimension=0, tiled=True)
    image_grad = back_unit(image_unit, image_norm, image_unit_grad)
    text_grad = back_unit(text_unit, text_norm, text_unit_grad)
    return (loss, image_grad, text_grad)


def fused_kernel(
    n_row, n_col, img_ref, txt_ref, match_ref, scale_ref, loss_ref, gimg_ref, gtxt_ref,
    raw, low, own, sc, ex, wbuf, stat, tile, lsem, ssem, rsem,
):
    per = img_ref.shape[0]
    n_dev = n_row * n_col
    total = per * n_dev
    units = raw.shape[1]
    width = 4 * per
    pair = 2 * per
    row = lax.axis_index("row")
    x = lax.axis_index("col")
    z, y, c = row // 4, (row // 2) % 2, row % 2
    me = row * n_col + x
    scale = scale_ref[0, 0]

    def place(zz, yy, cc, xx):
        return ((zz * 4 + yy * 2 + cc), xx)

    barrier = pltpu.get_barrier_semaphore()
    peers = [(me + k) % n_dev for k in range(1, n_dev)]
    peers = [(p // n_col, p % n_col) for p in peers]
    greet = [(row,1-x),(z*4+(1-y)*2+c,x),(z*4+y*2+1-c,x)]+[(((z+k)%4)*4+y*2+c,x) for k in (1,2,3)]
    for peer in greet:
        pl.semaphore_signal(barrier, inc=1, device_id=peer, device_id_type=MESH)

    inputs = (img_ref, txt_ref)
    kept = [
        pltpu.make_async_copy(inputs[a], raw.at[a, z * 2 + y, c * 2 + x], lsem.at[a])
        for a in range(2)
    ]
    for copy in kept:
        copy.start()
    for a in range(2):
        wide = inputs[a][...].astype(jnp.float32)
        norm = jnp.sqrt(jnp.sum(wide * wide, axis=1, keepdims=True) + EPSILON)
        own[a] = (wide * (1.0 / norm)).astype(jnp.bfloat16)
    for copy in kept:
        copy.wait()
    pl.semaphore_wait(barrier, len(greet))

    copies = []

    def send(src, dst, target):
        k = len(copies)
        copy = pltpu.make_async_remote_copy(
            src_ref=src, dst_ref=dst, send_sem=ssem.at[k], recv_sem=rsem.at[k],
            device_id=target, device_id_type=MESH,
        )
        copy.start()
        copies.append(copy)
        return copy

    def move(a, zz, yy, xx, target):
        ref = raw.at[a, zz * 2 + yy, c * 2 + xx]
        return send(ref, ref, target)

    to_x, to_y = place(z, y, c, 1 - x), place(z, 1 - y, c, x)
    sibling = place(z, y, 1 - c, x)

    def share(zz, yy, xx):
        ref = raw.at[:, zz * 2 + yy, c * 2 + xx]
        return send(ref, ref, sibling)

    def zmate(k):
        low_bit, high_bit = z % 2, z // 2
        if k & 1:
            low_bit = 1 - low_bit
        if k & 2:
            high_bit = 1 - high_bit
        return high_bit * 2 + low_bit

    zs = [zmate(k) for k in range(4)]

    def process(zz, yy):
        unit = zz * 2 + yy
        @pl.loop(0, 4)
        def _(b):
            for a in range(2):
                wide = raw[a, unit, b].astype(jnp.float32)
                norm = jnp.sqrt(jnp.sum(wide * wide, axis=1, keepdims=True) + EPSILON)
                rows = pl.ds(pl.multiple_of(unit * width + b * per, per), per)
                low[a, rows, :] = (wide * (1.0 / norm)).astype(jnp.bfloat16)

        rows = pl.ds(pl.multiple_of(unit * width, width), width)
        for a in range(2):
            sc[a, unit] = scale * lax.dot_general(
                own[1 - a], low[a, rows, :], (((1,), (1,)), ((), ())),
                preferred_element_type=jnp.float32,
            )

    lines = [None]
    first, second, third, shares = {}, {}, {}, {}

    def stage1(k):
        if k:
            for copy in lines[k]:
                copy.wait_recv()
        ax = move(0, zs[k], y, x, to_x)
        by = move(1, zs[k], y, x, to_y)
        bx = move(1, zs[k], y, x, to_x)
        ay = move(0, zs[k], y, x, to_y)
        first[k] = (ax, by)
        second[k] = (bx, ay)
        shares[k] = [share(zs[k], y, x)]

    def stage2(k):
        if k == 1:
            return
        ax, by = first[k]
        ax.wait_recv()
        ady = move(0, zs[k], y, 1 - x, to_y)
        by.wait_recv()
        bdx = move(1, zs[k], 1 - y, x, to_x)
        third[k] = (ady, bdx)

    def stage3(k):
        if k == 1:
            for copy in first[k]:
                copy.wait_recv()
        bx, ay = second[k]
        bx.wait_recv()
        shares[k].append(share(zs[k], y, 1 - x))
        ay.wait_recv()
        shares[k].append(share(zs[k], 1 - y, x))

    def stage4(k):
        for copy in third[k]:
            copy.wait_recv()
        if k == 0:
            corner = raw.at[:, z * 2 + 1 - y, c * 2 + 1 - x]
            third[1] = (send(corner, corner, place(zs[1], y, c, x)),)
        shares[k].append(share(zs[k], 1 - y, 1 - x))

    stage1(0)
    for k in range(1, 4):
        lines.append([move(a, z, y, x, place(zs[k], y, c, x)) for a in range(2)])
    stage2(0)
    for k in range(4):
        if k + 1 < 4:
            stage1(k + 1)
        stage3(k)
        shares[k][0].wait_recv()
        shares[k][1].wait_recv()
        process(zs[k], y)
        stage4(k)
        if k + 1 < 4:
            stage2(k + 1)
        shares[k][2].wait_recv()
        shares[k][3].wait_recv()
        process(zs[k], 1 - y)

    lane = lax.broadcasted_iota(jnp.int32, (per, pair), 1)
    sub = lax.broadcasted_iota(jnp.int32, (per, pair), 0)
    eye = lane == sub + x * per
    match_row = match_ref[...].astype(jnp.float32)
    match_own = jnp.sum(jnp.where(eye, match_row, 0.0), axis=1, keepdims=True)
    lses, sums = [None, None], [None, None]
    for a in range(2):
        top = jnp.max(sc[a, 0], axis=1, keepdims=True)
        for u in range(1, units):
            top = jnp.maximum(top, jnp.max(sc[a, u], axis=1, keepdims=True))
        acc = jnp.zeros((per, width), jnp.float32)
        for u in range(units):
            e = jnp.exp(sc[a, u] - top)
            ex[a, u] = e
            acc = acc + e
        sums[a] = jnp.sum(acc, axis=1, keepdims=True)
        lses[a] = top + jnp.log(sums[a])
    unit_lane = lax.broadcasted_iota(jnp.int32, (per, width), 1).astype(jnp.float32)
    hit = jnp.zeros((per, width), jnp.float32)
    for u in range(units):
        hit = hit + jnp.where(unit_lane + float(u * width) == match_own, sc[1, u], 0.0)
    matched = jnp.sum(jnp.sum(hit, axis=1, keepdims=True), axis=0, keepdims=True)

    def as_lanes(column):
        return jnp.sum(jnp.where(eye, column, 0.0), axis=0, keepdims=True)

    here = lax.broadcasted_iota(jnp.int32, (1, pair), 1)
    inside = (here >= x * per) & (here < (x + 1) * per)
    tile[0:1, :] = as_lanes(lses[1])
    tile[1:2, :] = as_lanes(lses[0])
    tile[2:3, :] = jnp.where(inside, match_row, 0.0)
    tile[3:4, :] = jnp.where(here == 0, matched, 0.0)
    tile[4:8, :] = jnp.zeros((4, pair), jnp.float32)
    stat[me] = tile[...]
    news = [send(tile, stat.at[me], peer) for peer in peers]

    for a in range(2):
        half = 0.5 / sums[a]
        for u in range(units):
            part = ex[a, u] * half
            if a == 1:
                part = part - jnp.where(unit_lane + float(u * width) == match_own, 1.0, 0.0)
            ex[a, u] = part

    for copy in news:
        copy.wait_recv()
    blocks = [stat[2 * k] + stat[2 * k + 1] for k in range(n_dev // 2)]
    everyone = blocks[0]
    for block in blocks[1:]:
        everyone = everyone + block
    rows8 = lax.broadcasted_iota(jnp.int32, everyone.shape, 0)
    factor = jnp.where(rows8 < 2, 0.5 / total, jnp.where(rows8 == 3, -1.0 / total, 0.0))
    loss_ref[...] = jnp.sum(
        jnp.sum(everyone * factor, axis=1, keepdims=True), axis=0, keepdims=True
    )
    text_id = (
        lax.broadcasted_iota(jnp.int32, (per, 1), 0) + me * per
    ).astype(jnp.float32)
    for a in (1, 0):
        for u in range(units):
            wide = jnp.concatenate([blocks[2 * u], blocks[2 * u + 1]], axis=1)
            other = wide[1:2, :] if a == 1 else wide[0:1, :]
            value = ex[a, u] + 0.5 * jnp.exp(sc[a, u] - other)
            if a == 0:
                value = value - jnp.where(wide[2:3, :] == text_id, 1.0, 0.0)
            wbuf[a, :, u * width : (u + 1) * width] = (scale * value).astype(jnp.bfloat16)
        grad = jnp.dot(wbuf[a], low[a], preferred_element_type=jnp.float32)
        source, out = (img_ref, gimg_ref) if a == 1 else (txt_ref, gtxt_ref)
        wide = source[...].astype(jnp.float32)
        norm = jnp.sqrt(jnp.sum(wide * wide, axis=1, keepdims=True) + EPSILON)
        inv = 1.0 / norm
        unit = wide * inv
        inner = jnp.sum(unit * grad, axis=1, keepdims=True)
        out[...] = (grad - unit * inner) * inv
    for copy in copies:
        copy.wait_send()


def fused(n_row, n_col, images, texts, matches, logit_scale):
    per, d = images.shape
    n_dev = n_row * n_col
    units = n_dev // 4
    n_sem = 6 + 10 * 4 + n_dev - 1
    vmem = pl.BlockSpec(memory_space=pltpu.VMEM)
    loss, image_grad, text_grad = pl.pallas_call(
        functools.partial(fused_kernel, n_row, n_col),
        out_shape=(
            jax.ShapeDtypeStruct((1, 1), jnp.float32),
            jax.ShapeDtypeStruct((per, d), jnp.float32),
            jax.ShapeDtypeStruct((per, d), jnp.float32),
        ),
        in_specs=[vmem, vmem, vmem, pl.BlockSpec(memory_space=pltpu.SMEM)],
        out_specs=(vmem, vmem, vmem),
        scratch_shapes=[
            pltpu.VMEM((2, units, 4, per, d), jnp.bfloat16),
            pltpu.VMEM((2, units * 4 * per, d), jnp.bfloat16),
            pltpu.VMEM((2, per, d), jnp.bfloat16),
            pltpu.VMEM((2, units, per, 4 * per), jnp.float32),
            pltpu.VMEM((2, units, per, 4 * per), jnp.float32),
            pltpu.VMEM((2, per, units * 4 * per), jnp.bfloat16),
            pltpu.VMEM((n_dev, 8, 2 * per), jnp.float32),
            pltpu.VMEM((8, 2 * per), jnp.float32),
            pltpu.SemaphoreType.DMA((2,)),
            pltpu.SemaphoreType.DMA((n_sem,)),
            pltpu.SemaphoreType.DMA((n_sem,)),
        ],
        compiler_params=pltpu.CompilerParams(
            collective_id=0, has_side_effects=True, vmem_limit_bytes=56 * 1024 * 1024
        ),
    )(images, texts, matches.reshape(1, -1), logit_scale.reshape(1, 1))
    return loss.reshape(()), image_grad, text_grad


def solution(mesh):
    placed = (P(("row", "col"), None), P(("row", "col"), None), P("row"), P())
    n_row, n_col = mesh.shape["row"], mesh.shape["col"]

    def body(images, texts, matches, logit_scale):
        if n_col == 2 and n_row == 16 and matches.shape[0] == 128:
            return fused(n_row, n_col, images, texts, matches, logit_scale)
        return on_device(images, texts, matches, logit_scale)

    return jax.shard_map(
        body,
        mesh=mesh,
        in_specs=placed,
        out_specs=(P(), P(("row", "col"), None), P(("row", "col"), None)),
        check_vma=False,
    )
```

```python
import functools

import jax
import jax.numpy as jnp
from jax import lax
from jax.experimental import pallas as pl
from jax.experimental.pallas import tpu as pltpu
from jax.sharding import PartitionSpec as P

EPSILON = 1e-06
MESH = pl.DeviceIdType.MESH


def merged(value, axis, join):
    pieces = jax.tree.map(lambda part: lax.all_gather(part, axis), value)
    head = jax.tree.map(lambda part: part[0], pieces)
    tail = jax.tree.map(lambda part: part[1:], pieces)
    running, _ = lax.scan(lambda running, piece: (join(running, piece), None), head, tail)
    return running


def unit_rows(values):
    wide = values.astype(jnp.float32)
    norms = jnp.sqrt(jnp.sum(wide * wide, axis=1, keepdims=True) + EPSILON)
    return (wide / norms, norms)


def back_unit(unit, norms, grad):
    inner = jnp.sum(unit * grad, axis=1, keepdims=True)
    return (grad - unit * inner) / norms


def combine_stats(first, second):
    top = jnp.maximum(first[0], second[0])
    return (top, first[1] * jnp.exp(first[0] - top) + second[1] * jnp.exp(second[0] - top))


def on_device(images, texts, matches, logit_scale):
    per_dev = images.shape[0]
    n_row = lax.axis_size("row")
    n_col = lax.axis_size("col")
    total = per_dev * n_row * n_col
    col_pos = lax.axis_index("col")
    row_pos = lax.axis_index("row")
    image_unit, image_norm = unit_rows(images)
    text_unit, text_norm = unit_rows(texts)
    image_low = image_unit.astype(jnp.bfloat16)
    text_low = text_unit.astype(jnp.bfloat16)
    image_rows = lax.all_gather(image_low, "col", axis=0, tiled=True)
    half = 0
    stride = 1
    n_img = image_rows.shape[0]

    def scores_of(piece):
        return logit_scale * lax.dot_general(
            piece, image_rows, (((1,), (1,)), ((), ())), preferred_element_type=jnp.float32
        )

    def match_mask(count):
        place = jnp.arange(count, dtype=jnp.int32)
        owner = place // per_dev * stride + half
        text_ids = owner * (n_col * per_dev) + col_pos * per_dev + place % per_dev
        return text_ids[:, None] == matches[None, :]

    piece = lax.all_gather(text_low, "row", axis=0, tiled=True)
    row_max = jnp.full((n_img,), -jnp.inf, jnp.float32)
    row_sum = jnp.zeros((n_img,), jnp.float32)
    scores = scores_of(piece)
    top = jnp.max(scores, axis=0)
    row_sum = row_sum * jnp.exp(row_max - top) + jnp.sum(jnp.exp(scores - top[None, :]), axis=0)
    piece_max = jnp.max(scores, axis=1)
    piece_sum = jnp.sum(jnp.exp(scores - piece_max[:, None]), axis=1)
    col_max = piece_max
    col_sum = piece_sum
    mask = match_mask(piece.shape[0])
    matched = jnp.sum(jnp.where(mask, scores, jnp.float32(0.0)))
    stats = (top, row_sum, col_max, col_sum, matched)
    row_max, row_sum, col_max, col_sum, matched = stats
    row_max, row_sum = merged((row_max, row_sum), "col", combine_stats)
    slot_max = col_max
    slot_sum = col_sum
    slot_max, slot_sum = merged((slot_max, slot_sum), "row", combine_stats)
    col_max = slot_max
    col_sum = slot_sum
    row_lse = row_max + jnp.log(row_sum)
    col_lse = col_max + jnp.log(col_sum)
    own_rows = jnp.sum(
        lax.dynamic_slice_in_dim(row_lse, (half * n_col + col_pos) * per_dev, per_dev, 0)
    )
    own_cols = jnp.sum(lax.dynamic_slice_in_dim(col_lse, row_pos // stride * per_dev, per_dev, 0))
    share = (own_rows + own_cols) / (2.0 * total) - matched / total
    loss = lax.psum(share, ("row", "col"))
    piece = lax.all_gather(text_low, "row", axis=0, tiled=True)
    count = piece.shape[0]
    scores = scores_of(piece)
    mask = match_mask(count).astype(jnp.float32)
    weights = (
        0.5 * jnp.exp(scores - row_lse[None, :]) + 0.5 * jnp.exp(scores - col_lse[:, None]) - mask
    )
    weights = (logit_scale * weights).astype(jnp.bfloat16)
    image_acc = lax.dot_general(
        weights, piece, (((0,), (0,)), ((), ())), preferred_element_type=jnp.float32
    )
    text_piece = jnp.dot(weights, image_rows, preferred_element_type=jnp.float32)
    text_acc = text_piece
    image_acc, text_acc = (image_acc, text_acc)
    image_unit_grad = lax.psum_scatter(image_acc, "col", scatter_dimension=0, tiled=True)
    text_unit_grad = lax.psum_scatter(text_acc, "row", scatter_dimension=0, tiled=True)
    image_grad = back_unit(image_unit, image_norm, image_unit_grad)
    text_grad = back_unit(text_unit, text_norm, text_unit_grad)
    return (loss, image_grad, text_grad)


def fused_kernel(
    n_row, n_col, img_ref, txt_ref, match_ref, scale_ref, loss_ref, gimg_ref, gtxt_ref,
    raw, low, own, sc, ex, wbuf, stat, tile, lsem, ssem, rsem,
):
    per = img_ref.shape[0]
    n_dev = n_row * n_col
    total = per * n_dev
    units = raw.shape[1]
    width = 4 * per
    pair = 2 * per
    row = lax.axis_index("row")
    x = lax.axis_index("col")
    z, y, c = row // 4, (row // 2) % 2, row % 2
    me = row * n_col + x
    scale = scale_ref[0, 0]

    def place(zz, yy, cc, xx):
        return ((zz * 4 + yy * 2 + cc), xx)

    barrier = pltpu.get_barrier_semaphore()
    peers = [(me + k) % n_dev for k in range(1, n_dev)]
    peers = [(p // n_col, p % n_col) for p in peers]
    greet = [(row,1-x),(z*4+(1-y)*2+c,x),(z*4+y*2+1-c,x)]+[(((z+k)%4)*4+y*2+c,x) for k in (1,2,3)]
    for peer in greet:
        pl.semaphore_signal(barrier, inc=1, device_id=peer, device_id_type=MESH)

    inputs = (img_ref, txt_ref)
    kept = [
        pltpu.make_async_copy(inputs[a], raw.at[a, z * 2 + y, c * 2 + x], lsem.at[a])
        for a in range(2)
    ]
    for copy in kept:
        copy.start()
    for a in range(2):
        wide = inputs[a][...].astype(jnp.float32)
        norm = jnp.sqrt(jnp.sum(wide * wide, axis=1, keepdims=True) + EPSILON)
        own[a] = (wide * (1.0 / norm)).astype(jnp.bfloat16)
    for copy in kept:
        copy.wait()
    pl.semaphore_wait(barrier, len(greet))

    copies = []

    def send(src, dst, target):
        k = len(copies)
        copy = pltpu.make_async_remote_copy(
            src_ref=src, dst_ref=dst, send_sem=ssem.at[k], recv_sem=rsem.at[k],
            device_id=target, device_id_type=MESH,
        )
        copy.start()
        copies.append(copy)
        return copy

    def move(a, zz, yy, xx, target):
        ref = raw.at[a, zz * 2 + yy, c * 2 + xx]
        return send(ref, ref, target)

    to_x, to_y = place(z, y, c, 1 - x), place(z, 1 - y, c, x)
    sibling = place(z, y, 1 - c, x)

    def share(zz, yy, xx):
        ref = raw.at[:, zz * 2 + yy, c * 2 + xx]
        return send(ref, ref, sibling)

    def zmate(k):
        low_bit, high_bit = z % 2, z // 2
        if k & 1:
            low_bit = 1 - low_bit
        if k & 2:
            high_bit = 1 - high_bit
        return high_bit * 2 + low_bit

    zs = [zmate(k) for k in (0, 1, 3, 2)]

    def process(zz, yy):
        unit = zz * 2 + yy
        @pl.loop(0, 4)
        def _(b):
            for a in range(2):
                wide = raw[a, unit, b].astype(jnp.float32)
                norm = jnp.sqrt(jnp.sum(wide * wide, axis=1, keepdims=True) + EPSILON)
                rows = pl.ds(pl.multiple_of(unit * width + b * per, per), per)
                low[a, rows, :] = (wide * (1.0 / norm)).astype(jnp.bfloat16)

        rows = pl.ds(pl.multiple_of(unit * width, width), width)
        for a in range(2):
            sc[a, unit] = scale * lax.dot_general(
                own[1 - a], low[a, rows, :], (((1,), (1,)), ((), ())),
                preferred_element_type=jnp.float32,
            )

    lines = [None]
    first, second, third, shares = {}, {}, {}, {}

    def stage1(k):
        if k:
            for copy in lines[k]:
                copy.wait_recv()
        ax = move(0, zs[k], y, x, to_x)
        by = move(1, zs[k], y, x, to_y)
        bx = move(1, zs[k], y, x, to_x)
        ay = move(0, zs[k], y, x, to_y)
        first[k] = (ax, by)
        second[k] = (bx, ay)
        shares[k] = [share(zs[k], y, x)]

    def stage2(k):
        if k == 1:
            return
        ax, by = first[k]
        ax.wait_recv()
        ady = move(0, zs[k], y, 1 - x, to_y)
        by.wait_recv()
        bdx = move(1, zs[k], 1 - y, x, to_x)
        third[k] = (ady, bdx)

    def stage3(k):
        if k == 1:
            for copy in first[k]:
                copy.wait_recv()
        bx, ay = second[k]
        bx.wait_recv()
        shares[k].append(share(zs[k], y, 1 - x))
        ay.wait_recv()
        shares[k].append(share(zs[k], 1 - y, x))

    def stage4(k):
        for copy in third[k]:
            copy.wait_recv()
        if k == 0:
            corner = raw.at[:, z * 2 + 1 - y, c * 2 + 1 - x]
            third[1] = (send(corner, corner, place(zs[1], y, c, x)),)
        shares[k].append(share(zs[k], 1 - y, 1 - x))

    stage1(0)
    for k in range(1, 4):
        lines.append([move(a, z, y, x, place(zs[k], y, c, x)) for a in range(2)])
    stage2(0)
    for k in range(4):
        if k + 1 < 4:
            stage1(k + 1)
        stage3(k)
        shares[k][0].wait_recv()
        shares[k][1].wait_recv()
        process(zs[k], y)
        stage4(k)
        if k + 1 < 4:
            stage2(k + 1)
        shares[k][2].wait_recv()
        shares[k][3].wait_recv()
        process(zs[k], 1 - y)

    lane = lax.broadcasted_iota(jnp.int32, (per, pair), 1)
    sub = lax.broadcasted_iota(jnp.int32, (per, pair), 0)
    eye = lane == sub + x * per
    match_row = match_ref[...].astype(jnp.float32)
    match_own = jnp.sum(jnp.where(eye, match_row, 0.0), axis=1, keepdims=True)
    lses, sums = [None, None], [None, None]
    for a in range(2):
        top = jnp.max(sc[a, 0], axis=1, keepdims=True)
        for u in range(1, units):
            top = jnp.maximum(top, jnp.max(sc[a, u], axis=1, keepdims=True))
        acc = jnp.zeros((per, width), jnp.float32)
        for u in range(units):
            e = jnp.exp(sc[a, u] - top)
            ex[a, u] = e
            acc = acc + e
        sums[a] = jnp.sum(acc, axis=1, keepdims=True)
        lses[a] = top + jnp.log(sums[a])
    unit_lane = lax.broadcasted_iota(jnp.int32, (per, width), 1).astype(jnp.float32)
    hit = jnp.zeros((per, width), jnp.float32)
    for u in range(units):
        hit = hit + jnp.where(unit_lane + float(u * width) == match_own, sc[1, u], 0.0)
    matched = jnp.sum(jnp.sum(hit, axis=1, keepdims=True), axis=0, keepdims=True)

    def as_lanes(column):
        return jnp.sum(jnp.where(eye, column, 0.0), axis=0, keepdims=True)

    here = lax.broadcasted_iota(jnp.int32, (1, pair), 1)
    inside = (here >= x * per) & (here < (x + 1) * per)
    tile[0:1, :] = as_lanes(lses[1])
    tile[1:2, :] = as_lanes(lses[0])
    tile[2:3, :] = jnp.where(inside, match_row, 0.0)
    tile[3:4, :] = jnp.where(here == 0, matched, 0.0)
    tile[4:8, :] = jnp.zeros((4, pair), jnp.float32)
    stat[me] = tile[...]
    news = [send(tile, stat.at[me], peer) for peer in peers]

    for a in range(2):
        half = 0.5 / sums[a]
        for u in range(units):
            part = ex[a, u] * half
            if a == 1:
                part = part - jnp.where(unit_lane + float(u * width) == match_own, 1.0, 0.0)
            ex[a, u] = part

    for copy in news:
        copy.wait_recv()
    blocks = [stat[2 * k] + stat[2 * k + 1] for k in range(n_dev // 2)]
    everyone = blocks[0]
    for block in blocks[1:]:
        everyone = everyone + block
    rows8 = lax.broadcasted_iota(jnp.int32, everyone.shape, 0)
    factor = jnp.where(rows8 < 2, 0.5 / total, jnp.where(rows8 == 3, -1.0 / total, 0.0))
    loss_ref[...] = jnp.sum(
        jnp.sum(everyone * factor, axis=1, keepdims=True), axis=0, keepdims=True
    )
    text_id = (
        lax.broadcasted_iota(jnp.int32, (per, 1), 0) + me * per
    ).astype(jnp.float32)
    for a in (1, 0):
        for u in range(units):
            wide = jnp.concatenate([blocks[2 * u], blocks[2 * u + 1]], axis=1)
            other = wide[1:2, :] if a == 1 else wide[0:1, :]
            value = ex[a, u] + 0.5 * jnp.exp(sc[a, u] - other)
            if a == 0:
                value = value - jnp.where(wide[2:3, :] == text_id, 1.0, 0.0)
            wbuf[a, :, u * width : (u + 1) * width] = (scale * value).astype(jnp.bfloat16)
        grad = jnp.dot(wbuf[a], low[a], preferred_element_type=jnp.float32)
        source, out = (img_ref, gimg_ref) if a == 1 else (txt_ref, gtxt_ref)
        wide = source[...].astype(jnp.float32)
        norm = jnp.sqrt(jnp.sum(wide * wide, axis=1, keepdims=True) + EPSILON)
        inv = 1.0 / norm
        unit = wide * inv
        inner = jnp.sum(unit * grad, axis=1, keepdims=True)
        out[...] = (grad - unit * inner) * inv
    for copy in copies:
        copy.wait_send()


def fused(n_row, n_col, images, texts, matches, logit_scale):
    per, d = images.shape
    n_dev = n_row * n_col
    units = n_dev // 4
    n_sem = 6 + 10 * 4 + n_dev - 1
    vmem = pl.BlockSpec(memory_space=pltpu.VMEM)
    loss, image_grad, text_grad = pl.pallas_call(
        functools.partial(fused_kernel, n_row, n_col),
        out_shape=(
            jax.ShapeDtypeStruct((1, 1), jnp.float32),
            jax.ShapeDtypeStruct((per, d), jnp.float32),
            jax.ShapeDtypeStruct((per, d), jnp.float32),
        ),
        in_specs=[vmem, vmem, vmem, pl.BlockSpec(memory_space=pltpu.SMEM)],
        out_specs=(vmem, vmem, vmem),
        scratch_shapes=[
            pltpu.VMEM((2, units, 4, per, d), jnp.bfloat16),
            pltpu.VMEM((2, units * 4 * per, d), jnp.bfloat16),
            pltpu.VMEM((2, per, d), jnp.bfloat16),
            pltpu.VMEM((2, units, per, 4 * per), jnp.float32),
            pltpu.VMEM((2, units, per, 4 * per), jnp.float32),
            pltpu.VMEM((2, per, units * 4 * per), jnp.bfloat16),
            pltpu.VMEM((n_dev, 8, 2 * per), jnp.float32),
            pltpu.VMEM((8, 2 * per), jnp.float32),
            pltpu.SemaphoreType.DMA((2,)),
            pltpu.SemaphoreType.DMA((n_sem,)),
            pltpu.SemaphoreType.DMA((n_sem,)),
        ],
        compiler_params=pltpu.CompilerParams(
            collective_id=0, has_side_effects=True, vmem_limit_bytes=56 * 1024 * 1024
        ),
    )(images, texts, matches.reshape(1, -1), logit_scale.reshape(1, 1))
    return loss.reshape(()), image_grad, text_grad


def solution(mesh):
    placed = (P(("row", "col"), None), P(("row", "col"), None), P("row"), P())
    n_row, n_col = mesh.shape["row"], mesh.shape["col"]

    def body(images, texts, matches, logit_scale):
        if n_col == 2 and n_row == 16 and matches.shape[0] == 128:
            return fused(n_row, n_col, images, texts, matches, logit_scale)
        return on_device(images, texts, matches, logit_scale)

    return jax.shard_map(
        body,
        mesh=mesh,
        in_specs=placed,
        out_specs=(P(), P(("row", "col"), None), P(("row", "col"), None)),
        check_vma=False,
    )
```
